32 devices in a mesh: seq: 2 (over core), ctx: 4 (over y, x), tp: 4 (over z).
Axes of the slice: x: 2, y: 2, z: 4, core: 2. Of those that a mesh axis runs over, the one named last changes fastest.
Arguments:
- queries: bfloat16 [2048, 16, 128], P(('seq', 'ctx'), 'tp'), parts along dimension 0, may hold values from -160 to 160
- key_rows: bfloat16 [2048, 4, 128], P(('seq', 'ctx'), 'tp'), parts along dimension 0, may hold values from -5 to 5
- value_slot_rows: bfloat16 [2048, 4, 128], P(('seq', 'ctx'), 'tp'), parts along dimension 0, may hold values from -6 to 6
- out_grad: bfloat16 [2048, 16, 128], P(('seq', 'ctx'), 'tp'), parts along dimension 0, may hold values from -6 to 6
- span_order: int32 [16], P('seq'), parts along dimension 0, may hold values from 0 to 7, each once
Outputs:
- query_grad: bfloat16 [2048, 16, 128], P(('seq', 'ctx'), 'tp'), parts along dimension 0
- key_gradient: bfloat16 [2048, 4, 128], P(('seq', 'ctx'), 'tp'), parts along dimension 0
- value_gradient: bfloat16 [2048, 4, 128], P(('seq', 'ctx'), 'tp'), parts along dimension 0
The draws below stay inside these ranges and needn't reach their ends.
There are 2 independent parts, one for each index of `seq`. The reference program is written for one: setup_inputs(seed, part) draws one part's arguments, and reference() takes and returns one part's arrays. A program takes and returns all parts, laid end to end along the dimension named above; each array names one. Nothing has to cross between parts.
Inputs may be any that keep to these rules, and one draw needn't show every extreme that they name: Slot s of 128 rows holds span span_order[s] of the sequence; every span number stands once.
All inputs are finite; a program needn't handle non-finite values.
Results may differ from the reference program's by a relative error of at most 0.0085.
Values may be sent and summed in bfloat16 or wider, within the bound.
A program may use at most 64 MiB of HBM per device.

```python
import math
import jax
import jax.numpy as jnp
from jax import lax

HEAD_SIZE = 128
QUERY_HEADS = 16
KEY_VALUE_HEADS = 4
SPAN = 128
SLOTS = 8
SEQUENCE_TOKENS = 1024


def keys_base(key):
    return jax.random.truncated_normal(jax.random.fold_in(key, 7), -5.0, 5.0, (SEQUENCE_TOKENS, KEY_VALUE_HEADS, HEAD_SIZE), jnp.float32)


def draw_key_rows(key, part):
    values = keys_base(key)
    return values.astype(jnp.bfloat16)


def draw_queries(key, part):
    values = jax.random.truncated_normal(jax.random.fold_in(key, 11), -5.0, 5.0, (SEQUENCE_TOKENS, QUERY_HEADS, HEAD_SIZE), jnp.float32)
    return values.astype(jnp.bfloat16)


def steps_of(key, extent, cuts, smallest, top_value):
    def one(position, shards_of):
        draws = jax.random.uniform(jax.random.fold_in(jax.random.fold_in(key, 6), position), (shards_of,), jnp.float32, smallest / len(cuts), top_value / len(cuts))
        return jnp.repeat(jnp.exp(draws), extent[position] // shards_of).reshape((-1,) + (1,) * (len(extent) - position - 1))

    loudness = one(*cuts[0])
    for cut in cuts[1:]:
        loudness = loudness * one(*cut)
    return loudness


def scatter_about(key, dims, spread, bound, pieces=(), held_as=jnp.bfloat16):
    result = spread * jax.random.normal(key, dims, jnp.float32)
    if pieces:
        result = result * steps_of(key, dims, pieces, -0.22, 0.18)
    return jnp.clip(result, -bound, bound).astype(held_as)


def setup_inputs(seed: int = 0, part: int = 0) -> dict:
    key_list = jax.random.split(jax.random.key(seed), 6)
    own_keys = jax.random.split(jax.random.fold_in(key_list[5], part), 6)
    return {
        "queries": draw_queries(jax.random.fold_in(jax.random.fold_in(key_list[5], part), 71), part),
        "key_rows": draw_key_rows(jax.random.fold_in(jax.random.fold_in(key_list[5], part), 71), part),
        "value_slot_rows": scatter_about(own_keys[2], (SEQUENCE_TOKENS, KEY_VALUE_HEADS, HEAD_SIZE), 1.0, 6.0, ((0, 4), (1, 4))),
        "out_grad": scatter_about(own_keys[3], (SEQUENCE_TOKENS, QUERY_HEADS, HEAD_SIZE), 1.0, 6.0, ((0, 4), (1, 4))),
        "span_order": jax.random.permutation(own_keys[4], SLOTS).astype(jnp.int32),
    }


NEGATIVE = -1e+30

def positions_of(span_order):
    offsets = jnp.tile(jnp.arange(SPAN, dtype=jnp.int32), SLOTS)
    return (jnp.repeat(span_order.astype(jnp.int32), SPAN) * SPAN + offsets).astype(jnp.int32)

def head_grads(query_head, key_head, value_head, grad_head, places):
    scaling = 1.0 / math.sqrt(HEAD_SIZE)
    value_wide = value_head.astype(jnp.float32)

    def step(carried, block_index):
        key_acc, value_acc = carried
        begin = (block_index * SPAN).astype(jnp.int32)
        q_block = lax.dynamic_slice_in_dim(query_head, begin, SPAN, 0)
        g_block = lax.dynamic_slice_in_dim(grad_head, begin, SPAN, 0)
        q_places = lax.dynamic_slice_in_dim(places, begin, SPAN, 0)
        visible = q_places[:, None] >= places[None, :]
        scores = jnp.dot(q_block, key_head.T, preferred_element_type=jnp.float32) * scaling
        scores = jnp.where(visible, scores, NEGATIVE)
        row_top = lax.optimization_barrier(jnp.max(scores, axis=1, keepdims=True))
        row_sum = lax.optimization_barrier(jnp.sum(jnp.where(visible, jnp.exp(scores - row_top), 0.0), axis=1, keepdims=True))
        log_total = row_top + jnp.log(row_sum)
        probs = jnp.where(visible, jnp.exp(scores - log_total), 0.0)
        probs_low = probs.astype(jnp.bfloat16)
        output = jnp.dot(probs, value_wide, precision=lax.Precision.HIGHEST, preferred_element_type=jnp.float32)
        row_delta = lax.optimization_barrier(jnp.sum(g_block.astype(jnp.float32) * output, axis=1, keepdims=True))
        grad_probs = jnp.dot(g_block, value_head.T, preferred_element_type=jnp.float32)
        grad_scores = (probs * (grad_probs - row_delta) * scaling).astype(jnp.bfloat16)
        query_part = jnp.dot(grad_scores, key_head, preferred_element_type=jnp.float32).astype(jnp.bfloat16)
        key_acc = key_acc + jnp.dot(grad_scores.T, q_block, preferred_element_type=jnp.float32)
        value_acc = value_acc + jnp.dot(probs_low.T, g_block, preferred_element_type=jnp.float32)
        return ((key_acc, value_acc), query_part)
    zeros = jnp.zeros((SEQUENCE_TOKENS, HEAD_SIZE), jnp.float32)
    (key_acc, value_acc), query_parts = lax.scan(step, (zeros, zeros), jnp.arange(SEQUENCE_TOKENS // SPAN, dtype=jnp.int32))
    return (query_parts.reshape(SEQUENCE_TOKENS, HEAD_SIZE), key_acc, value_acc)

def reference(queries, key_rows, value_slot_rows, out_grad, span_order):
    places = positions_of(span_order)
    query_cluster = QUERY_HEADS // KEY_VALUE_HEADS

    def per_head(head):
        kv_head = head // query_cluster
        query_head = lax.dynamic_index_in_dim(queries, head, 1, keepdims=False)
        grad_head = lax.dynamic_index_in_dim(out_grad, head, 1, keepdims=False)
        key_head = lax.dynamic_index_in_dim(key_rows, kv_head, 1, keepdims=False)
        value_head = lax.dynamic_index_in_dim(value_slot_rows, kv_head, 1, keepdims=False)
        return head_grads(query_head, key_head, value_head, grad_head, places)
    query_all, key_complete, value_complete = lax.map(per_head, jnp.arange(QUERY_HEADS, dtype=jnp.int32))
    query_grad = jnp.transpose(query_all, (1, 0, 2))
    key_gradient = jnp.transpose(key_complete.reshape(KEY_VALUE_HEADS, query_cluster, SEQUENCE_TOKENS, HEAD_SIZE).sum(axis=1), (1, 0, 2)).astype(jnp.bfloat16)
    value_gradient = jnp.transpose(value_complete.reshape(KEY_VALUE_HEADS, query_cluster, SEQUENCE_TOKENS, HEAD_SIZE).sum(axis=1), (1, 0, 2)).astype(jnp.bfloat16)
    return (query_grad, key_gradient, value_gradient)
```

```python
import functools
import math

import jax
import jax.numpy as jnp
from jax import lax
from jax.experimental import pallas as pl
from jax.experimental.pallas import tpu as pltpu
from jax.sharding import PartitionSpec as P

NEGATIVE = -1e30
MESH = pl.DeviceIdType.MESH
KEY_PIECES, VALUE_PIECES, BACK_PIECES = 1, 1, 1


def partner(me, o, n):
    total, bit = 0, 1
    while bit < n:
        total = total + (((me // bit) % 2 + (o // bit) % 2) % 2) * bit
        bit *= 2
    return total


def each(lo, hi, body):
    if hi - lo <= 4:
        for i in range(lo, hi):
            body(i)
    else:
        lax.fori_loop(lo, hi, lambda i, c: (body(i), c)[1], 0)


def dot(a, b, dims):
    return lax.dot_general(a, b, (dims, ((), ())), preferred_element_type=jnp.float32)


def square(cluster, slots_here, chunk, span_hbm, q_hbm, g_hbm, k_hbm, v_hbm,
           dq_ref, dk_ref, dv_ref,
           qg, kv, p, dp, ds, pb, part, recv, passing, held, top, total, dsum, delta, rank, acc, span_ref,
           load_sem, sent, first, second, third, pass_sem, home):
    n = 4
    me = lax.axis_index("ctx")
    rows = kv.shape[2]
    half_rows = rows // 2
    slot_rows = rows // slots_here
    cols, head_dim = qg.shape[1:]
    slot_cols = slot_rows * cluster
    chunks = cols // chunk
    scale = 1.0 / math.sqrt(head_dim)
    scale2 = scale * math.log2(math.e)
    q, g = qg.at[0], qg.at[1]
    pieces_of = (KEY_PIECES, VALUE_PIECES)

    load_k = pltpu.make_async_copy(k_hbm, kv.at[0, 0], load_sem.at[0])
    load_v = pltpu.make_async_copy(v_hbm, kv.at[0, 1], load_sem.at[1])
    load_span = pltpu.make_async_copy(span_hbm, span_ref, load_sem.at[2])
    load_qg = [pltpu.make_async_copy(src, dst, load_sem.at[3]) for src, dst in ((q_hbm, q), (g_hbm, g))]
    load_k.start()
    load_v.start()
    barrier = pltpu.get_barrier_semaphore()
    for o in (1, 2):
        pl.semaphore_signal(
            barrier, inc=1, device_id={"ctx": partner(me, o, n)}, device_id_type=MESH)
    load_span.start()
    for load in load_qg:
        load.start()
    rank[...] = lax.broadcasted_iota(jnp.int32, rank.shape, 0) - (
        lax.broadcasted_iota(jnp.int32, rank.shape, 1) // cluster)

    def remote(src, dst, sem, to):
        return pltpu.make_async_remote_copy(
            src_ref=src, dst_ref=dst, send_sem=sent.at[0], recv_sem=sem,
            device_id={"ctx": partner(me, to, n)}, device_id_type=MESH)

    def landed(ref, sem):
        pltpu.make_async_copy(ref, ref, sem).wait()

    def cut(h, c=0, pieces=1):
        size = half_rows // pieces
        return pl.ds(h * half_rows + c * size, size)

    def direct_first(o, which, c):
        at = cut(o - 1, c, pieces_of[which])
        return remote(kv.at[0, which, at], kv.at[o, which, at], first.at[which, o - 1, c], o)

    def direct_second(o, which):
        at = cut(2 - o)
        return remote(kv.at[0, which, at], kv.at[o, which, at], second.at[which], o)

    def relay(o, which, c):
        at = cut(2 - o, c, pieces_of[which])
        return remote(kv.at[3 - o, which, at], kv.at[3, which, at], third.at[which], o)

    def pass_gathered(which):
        for c in range(pieces_of[which]):
            for o in (1, 2):
                direct_first(3 - o, which, c).wait_recv()
                relay(o, which, c).start()

    def place(j):
        return pl.ds(j * slot_rows, slot_rows)

    def line(o, j):
        return pl.ds(o * slots_here + j, 1)

    def raw_scores(c, o, j):
        return dot(kv[o, 0, place(j)], q[pl.ds(c * chunk, chunk), :], ((1,), (1,)))

    def soften(c, o, j, piece):
        span = pl.ds(c * chunk, chunk)
        i = (c * chunk) // slot_cols
        shift = ((c * chunk) % slot_cols) // cluster
        diagonal = o == 0 and j == i
        if diagonal:
            piece = jnp.where(rank[...] <= shift, piece, NEGATIVE)
        peak = jnp.max(piece, axis=0, keepdims=True)
        e = jnp.exp2((piece - peak) * scale2)
        total[line(o, j), span] = jnp.sum(e, axis=0, keepdims=True)
        p[o, place(j), span] = e
        peak = peak * scale2
        if not diagonal:
            visible = span_ref[partner(me, o, n) * slots_here + j] < span_ref[me * slots_here + i]
            peak = jnp.where(visible, peak, NEGATIVE)
        top[line(o, j), span] = peak

    def scores(*blocks):
        for c in range(chunks):
            for o in blocks:
                for j in range(slots_here):
                    soften(c, o, j, raw_scores(c, o, j))

    def weigh(c, o):
        span = pl.ds(c * chunk, chunk)
        t = top[:, span]
        factor = jnp.exp2(t - jnp.max(t, axis=0, keepdims=True))
        weight = factor / jnp.sum(factor * total[:, span], axis=0, keepdims=True)
        top[:, span] = weight
        shares = []
        for j in range(slots_here):
            at = o * slots_here + j
            w = (p[o, place(j), span] * weight[at:at + 1]).astype(jnp.bfloat16)
            shares.append(dot(w, g[span, :], ((1,), (0,))))
        return shares

    def last_block(o):
        parts = None
        raw = [[raw_scores(c, o, j) for j in range(slots_here)] for c in range(chunks)]
        for c in range(chunks):
            for j in range(slots_here):
                soften(c, o, j, raw[c][j])
        for c in range(chunks):
            shares = weigh(c, o)
            parts = shares if parts is None else [a + b for a, b in zip(parts, shares)]
        return parts

    def products(*blocks):
        for c in range(chunks):
            span = pl.ds(c * chunk, chunk)
            for o in blocks:
                for j in range(slots_here):
                    d = dot(kv[o, 1, place(j)], g[span, :], ((1,), (1,)))
                    dsum[line(o, j), span] = jnp.sum(p[o, place(j), span] * d, axis=0, keepdims=True)
                    dp[o, place(j), span] = d

    def value_parts(*blocks):
        for c in range(chunks):
            span = pl.ds(c * chunk, chunk)
            for i, o in enumerate(blocks):
                for j in range(slots_here):
                    w = p[o, place(j), span] * top[line(o, j), span]
                    pb[i, place(j), span] = w.astype(jnp.bfloat16)
        return [[dot(pb[i, place(j)], g[...], ((1,), (0,))) for j in range(slots_here)]
                for i in range(len(blocks))]

    def key_parts(*blocks):
        for c in range(chunks):
            span = pl.ds(c * chunk, chunk)
            for o in blocks:
                for j in range(slots_here):
                    w = p[o, place(j), span] * top[line(o, j), span]
                    ds[o, place(j), span] = (
                        w * (dp[o, place(j), span] - delta[:, span])).astype(jnp.bfloat16)
        return [[dot(ds[o, place(j)], q[...], ((1,), (0,))) * scale for j in range(slots_here)]
                for o in blocks]

    def back_whole(o, which):
        return remote(part.at[o, which], recv.at[o, which], home.at[which], o)

    def back_piece(o, which, h, c=0, pieces=1):
        at = cut(h, c, pieces)
        return remote(part.at[o, which, at], recv.at[o, which, at], home.at[which], o)

    def back_diagonal(which, h, c):
        size = half_rows // BACK_PIECES
        return remote(part.at[3, which, cut(h, c, BACK_PIECES)],
                      passing.at[which, c, pl.ds(h * size, size)], pass_sem.at[which, c], 1 + h)

    def leave(which, direct, blocks, parts):
        sends = []
        for o, block in zip(blocks, parts):
            if direct or o == 3:
                for j in range(slots_here):
                    part[o, which, place(j)] = block[j].astype(part.dtype)
                sends += [back_whole(o, which)] if direct else [
                    back_diagonal(which, h, c) for c in range(BACK_PIECES) for h in (0, 1)]
            else:
                block = jnp.concatenate(block, axis=0)
                now, later = o - 1, 2 - o
                part[o, which, cut(now)] = block[now * half_rows:(now + 1) * half_rows].astype(part.dtype)
                held[o - 1, which] = block[later * half_rows:(later + 1) * half_rows]
                sends.append(back_piece(o, which, now))
        for send in sends:
            send.start()

    def pass_on(which):
        size = half_rows // BACK_PIECES
        for c in range(BACK_PIECES):
            landed(passing.at[which, c], pass_sem.at[which, c])
            for o in (1, 2):
                h = 2 - o
                part[o, which, cut(h, c, BACK_PIECES)] = (
                    held[o - 1, which, pl.ds(c * size, size)]
                    + passing[which, c, pl.ds(h * size, size)].astype(jnp.float32)).astype(part.dtype)
            for o in (1, 2):
                back_piece(o, which, 2 - o, c, BACK_PIECES).start()

    def store_own(which, block):
        for j in range(slots_here):
            acc[which, place(j)] = block[j]

    def plan(direct):
        pl.semaphore_wait(barrier, 2)
        for which, load in ((0, load_k), (1, load_v)):
            load.wait()
            for c in range(pieces_of[which]):
                for o in (1, 2):
                    direct_first(o, which, c).start()
        for which in range(2):
            for o in (1, 2):
                direct_second(o, which).start()
        load_span.wait()
        landed(qg, load_sem.at[3])
        scores(0)
        products(0)
        pass_gathered(0)
        pass_gathered(1)
        landed(kv.at[0, 0], second.at[0])
        scores(1, 2)
        landed(kv.at[0, 1], second.at[1])
        products(1, 2)
        landed(kv.at[3, 0], third.at[0])
        leave(1, direct[1], (3,), [last_block(3)])
        leave(1, direct[1], (1, 2), value_parts(1, 2))
        landed(kv.at[3, 1], third.at[1])
        products(3)
        delta[...] = jnp.sum(top[...] * dsum[...], axis=0, keepdims=True)
        leave(0, direct[0], (3,), key_parts(3))
        leave(0, direct[0], (1, 2), key_parts(1, 2))
        store_own(1, value_parts(0)[0])
        if not direct[1]:
            pass_on(1)
        store_own(0, key_parts(0)[0])
        if not direct[0]:
            pass_on(0)
        for c in range(chunks):
            span = pl.ds(c * chunk, chunk)
            sofar = jnp.zeros((head_dim, chunk), jnp.float32)
            for o in range(n):
                sofar = sofar + dot(kv[o, 0], ds[o, :, span], ((0,), (0,)))
            dq_ref[span, :] = (sofar.T * scale).astype(dq_ref.dtype)

        for which, out in ((1, dv_ref), (0, dk_ref)):
            count = 3 if direct[which] else 2
            landed(recv.at[pl.ds(1, count), which], home.at[which])
            whole = acc[which]
            for o in range(1, count + 1):
                whole = whole + recv[o, which].astype(jnp.float32)
            out[...] = whole.astype(out.dtype)
        landed(p.at[0, pl.ds(0, 12 * rows * head_dim * 2 // (4 * cols))], sent.at[0])

    lower = lax.axis_index("seq") % 2 == 0
    pl.when(lower)(lambda: plan((True, False)))
    pl.when(jnp.logical_not(lower))(lambda: plan((False, False)))


def kernel(n, cluster, slots_here, chunk, keep, span_hbm, q_hbm, g_hbm, k_hbm, v_hbm,
           dq_ref, dk_ref, dv_ref,
           q, g, kv, p, dp, ds, pb, part, recv, top, total, dsum, delta, rank, acc, span_ref,
           load_sem, send_sem, recv_sem, back_send, back_recv):
    me = lax.axis_index("ctx")
    rows = kv.shape[2]
    slot_rows = rows // slots_here
    cols = q.shape[0]
    slot_cols = slot_rows * cluster
    chunks = cols // chunk
    scale = 1.0 / math.sqrt(q.shape[1])
    scale2 = scale * math.log2(math.e)

    loads = [
        pltpu.make_async_copy(src, dst, load_sem.at[i])
        for i, (src, dst) in enumerate(
            [(k_hbm, kv.at[0, 0]), (v_hbm, kv.at[0, 1]), (q_hbm, q), (g_hbm, g),
             (span_hbm, span_ref)]
        )
    ]
    for load in loads:
        load.start()
    barrier = pltpu.get_barrier_semaphore()
    each(1, n, lambda o: pl.semaphore_signal(
        barrier, inc=1, device_id={"ctx": partner(me, o, n)}, device_id_type=MESH))
    rank[...] = lax.broadcasted_iota(jnp.int32, rank.shape, 0) - (
        lax.broadcasted_iota(jnp.int32, rank.shape, 1) // cluster)

    def remote(src, dst, sems, o, which):
        return pltpu.make_async_remote_copy(
            src_ref=src, dst_ref=dst,
            send_sem=sems[0].at[o, which], recv_sem=sems[1].at[o, which],
            device_id={"ctx": partner(me, o, n)}, device_id_type=MESH)

    there, home = (send_sem, recv_sem), (back_send, back_recv)

    def gather(o, which):
        return remote(kv.at[0, which], kv.at[o, which], there, o, which)

    def back(o, which):
        return remote(part.at[o, which], recv.at[o, which], home, o, which)

    def scores(o):
        source = partner(me, o, n)
        for c in range(chunks):
            span = pl.ds(c * chunk, chunk)
            s = dot(kv[o, 0], q[span, :], ((1,), (1,))) * scale2
            own = span_ref[me * slots_here + (c * chunk) // slot_cols]
            shift = ((c * chunk) % slot_cols) // cluster
            pieces = []
            for j in range(slots_here):
                limit = (own - span_ref[source * slots_here + j]) * slot_rows + shift
                pieces.append(jnp.where(
                    rank[...] <= limit, s[j * slot_rows:(j + 1) * slot_rows], NEGATIVE))
            s = jnp.concatenate(pieces, axis=0)
            m = jnp.max(s, axis=0, keepdims=True)
            e = jnp.exp2(s - m)
            top[o, :, span] = m
            total[o, :, span] = jnp.sum(e, axis=0, keepdims=True)
            p[o, :, span] = e.astype(p.dtype)

    def products(o):
        for c in range(chunks):
            span = pl.ds(c * chunk, chunk)
            d = dot(kv[o, 1], g[span, :], ((1,), (1,)))
            dsum[o, :, span] = jnp.sum(p[o, :, span].astype(jnp.float32) * d, axis=0, keepdims=True)
            if keep:
                dp[o, :, span] = d

    def normalize():
        factor = jnp.exp2(top[...] - jnp.max(top[...], axis=0)[None])
        whole = jnp.sum(factor * total[...], axis=0)
        top[...] = factor / whole[None]

    def value_part(o):
        for c in range(chunks):
            span = pl.ds(c * chunk, chunk)
            w = p[o, :, span].astype(jnp.float32) * top[o, :, span]
            pb[:, span] = w.astype(jnp.bfloat16)
        return dot(pb[...], g[...], ((1,), (0,)))

    def key_part(o):
        for c in range(chunks):
            span = pl.ds(c * chunk, chunk)
            w = p[o, :, span].astype(jnp.float32) * top[o, :, span]
            d = dp[o, :, span] if keep else dot(kv[o, 1], g[span, :], ((1,), (1,)))
            ds[o, :, span] = (w * (d - delta[:, span])).astype(jnp.bfloat16)
        return dot(ds[o], q[...], ((1,), (0,))) * scale

    def leave(o, which):
        part[o, which] = (key_part, value_part)[which](o).astype(part.dtype)
        back(o, which).start()

    pl.semaphore_wait(barrier, n - 1)
    for which in range(2):
        loads[which].wait()
        each(1, n, lambda o: gather(o, which).start())
    loads[4].wait()
    loads[2].wait()
    loads[3].wait()
    scores(0)
    products(0)

    def arrive(o):
        gather(o, 0).wait_recv()
        scores(o)
        gather(o, 1).wait_recv()
        products(o)

    each(1, n, arrive)
    normalize()
    each(1, n, lambda i: leave(n - i, 1))
    delta[...] = jnp.sum(top[...] * dsum[...], axis=0)
    each(1, n, lambda i: leave(n - i, 0))
    acc[1] = value_part(0)
    acc[0] = key_part(0)

    for c in range(chunks):
        span = pl.ds(c * chunk, chunk)

        def add(o, sofar):
            return sofar + dot(kv[o, 0], ds[o, :, span], ((0,), (0,)))

        sofar = jnp.zeros((q.shape[1], chunk), jnp.float32)
        if n <= 4:
            for o in range(n):
                sofar = add(o, sofar)
        else:
            sofar = lax.fori_loop(0, n, add, sofar)
        dq_ref[span, :] = (sofar.T * scale).astype(dq_ref.dtype)

    def collect(which):
        def one(o):
            back(o, which).wait_recv()
            acc[which] += recv[o, which].astype(jnp.float32)

        each(1, n, one)

    collect(1)
    dv_ref[...] = acc[1].astype(dv_ref.dtype)
    collect(0)
    dk_ref[...] = acc[0].astype(dk_ref.dtype)

    def finish(o):
        for which in range(2):
            gather(o, which).wait_send()
            back(o, which).wait_send()

    each(1, n, finish)


def store(dq, dk, dv, dq_out, dk_out, dv_out, sem):
    copies = [
        pltpu.make_async_copy(src, dst, sem.at[i])
        for i, (src, dst) in enumerate([(dq, dq_out), (dk, dk_out), (dv, dv_out)])
    ]
    for copy in copies:
        copy.start()
    for copy in copies:
        copy.wait()


def local(queries, key_rows, value_slot_rows, out_grad, span_order):
    rows, query_local, head_dim = queries.shape
    kv_local = key_rows.shape[1]
    assert kv_local == 1
    n = lax.axis_size("ctx")
    slots_here = span_order.shape[0] // n
    cluster = query_local // kv_local
    cols = rows * cluster
    chunk = math.gcd(256, cols // slots_here)
    keep = n <= 8
    slot_rows = rows // slots_here
    any_spec = pl.BlockSpec(memory_space=pl.ANY)
    vmem_spec = pl.BlockSpec(memory_space=pltpu.VMEM)
    bf16, f32 = jnp.bfloat16, jnp.float32
    pair = (n, 2, rows, head_dim)
    stat = (n * slots_here, cols) if n == 4 else (n, 1, cols)
    both = [pltpu.VMEM((2, cols, head_dim), bf16)] if n == 4 else [pltpu.VMEM((cols, head_dim), bf16)] * 2
    buffers = both + [
        pltpu.VMEM(pair, bf16),
        pltpu.VMEM((n, rows, cols), f32 if keep else bf16),
        pltpu.VMEM((n, rows, cols) if keep else (1, 8, 128), f32),
        pltpu.VMEM((n, rows, cols), bf16),
        pltpu.VMEM((2, rows, cols) if n == 4 else (rows, cols), bf16),
        pltpu.VMEM(pair, bf16),
        pltpu.VMEM(pair, bf16),
    ]
    sums = [
        pltpu.VMEM(stat, f32),
        pltpu.VMEM(stat, f32),
        pltpu.VMEM(stat, f32),
        pltpu.VMEM((1, cols), f32),
        pltpu.VMEM((slot_rows, chunk), jnp.int32),
        pltpu.VMEM((2, rows, head_dim), f32),
        pltpu.SMEM(span_order.shape, jnp.int32),
    ]
    dma = pltpu.SemaphoreType.DMA
    if n == 4:
        body = functools.partial(square, cluster, slots_here, chunk)
        scratch = buffers + [
            pltpu.VMEM((2, BACK_PIECES, rows // BACK_PIECES, head_dim), bf16),
            pltpu.VMEM((2, 2, rows // 2, head_dim), f32),
        ] + sums + [
            dma((4,)), dma((1,)), dma((2, 2, max(KEY_PIECES, VALUE_PIECES))), dma((2,)), dma((2,)),
            dma((2, BACK_PIECES)), dma((2,)),
        ]
    else:
        body = functools.partial(kernel, n, cluster, slots_here, chunk, keep)
        scratch = buffers + sums + [dma((5,))] + [dma((n, 2))] * 4
    dq, dk, dv = pl.pallas_call(
        body,
        out_shape=(
            pltpu.VMEM((cols, head_dim), bf16),
            pltpu.VMEM((rows, head_dim), bf16),
            pltpu.VMEM((rows, head_dim), bf16),
        ),
        in_specs=[any_spec] * 5,
        out_specs=(vmem_spec,) * 3,
        scratch_shapes=scratch,
        compiler_params=pltpu.CompilerParams(
            collective_id=0, has_side_effects=True, vmem_limit_bytes=60 * 1024 * 1024
        ),
    )(
        span_order,
        queries.reshape(cols, head_dim),
        out_grad.reshape(cols, head_dim),
        key_rows.reshape(rows, head_dim),
        value_slot_rows.reshape(rows, head_dim),
    )
    dq, dk, dv = pl.pallas_call(
        store,
        out_shape=tuple(jax.ShapeDtypeStruct(a.shape, bf16) for a in (dq, dk, dv)),
        in_specs=[vmem_spec] * 3,
        out_specs=(any_spec,) * 3,
        scratch_shapes=[pltpu.SemaphoreType.DMA((3,))],
    )(*(pltpu.with_memory_space_constraint(a, pltpu.VMEM) for a in (dq, dk, dv)))
    return dq.reshape(queries.shape), dk.reshape(key_rows.shape), dv.reshape(key_rows.shape)


def solution(mesh):
    rows = P(("seq", "ctx"), "tp", None)
    return jax.shard_map(
        local,
        mesh=mesh,
        in_specs=(rows, rows, rows, rows, P("seq")),
        out_specs=(rows, rows, rows),
        check_vma=False,
    )
```

```python
import functools
import math

import jax
import jax.numpy as jnp
from jax import lax
from jax.experimental import pallas as pl
from jax.experimental.pallas import tpu as pltpu
from jax.sharding import PartitionSpec as P

NEGATIVE = -1e30
MESH = pl.DeviceIdType.MESH
KEY_PIECES, VALUE_PIECES, BACK_PIECES = 2, 1, 2


def partner(me, o, n):
    total, bit = 0, 1
    while bit < n:
        total = total + (((me // bit) % 2 + (o // bit) % 2) % 2) * bit
        bit *= 2
    return total


def each(lo, hi, body):
    if hi - lo <= 4:
        for i in range(lo, hi):
            body(i)
    else:
        lax.fori_loop(lo, hi, lambda i, c: (body(i), c)[1], 0)


def dot(a, b, dims):
    return lax.dot_general(a, b, (dims, ((), ())), preferred_element_type=jnp.float32)


def square(cluster, slots_here, chunk, span_hbm, q_hbm, g_hbm, k_hbm, v_hbm,
           dq_ref, dk_ref, dv_ref,
           qg, kv, p, dp, ds, pb, part, recv, passing, held, top, total, dsum, delta, rank, acc, span_ref,
           load_sem, sent, first, second, third, pass_sem, home):
    n = 4
    me = lax.axis_index("ctx")
    rows = kv.shape[2]
    half_rows = rows // 2
    slot_rows = rows // slots_here
    cols, head_dim = qg.shape[1:]
    slot_cols = slot_rows * cluster
    chunks = cols // chunk
    scale = 1.0 / math.sqrt(head_dim)
    scale2 = scale * math.log2(math.e)
    q, g = qg.at[0], qg.at[1]
    pieces_of = (KEY_PIECES, VALUE_PIECES)

    load_k = pltpu.make_async_copy(k_hbm, kv.at[0, 0], load_sem.at[0])
    load_v = pltpu.make_async_copy(v_hbm, kv.at[0, 1], load_sem.at[1])
    load_span = pltpu.make_async_copy(span_hbm, span_ref, load_sem.at[2])
    load_qg = [pltpu.make_async_copy(src, dst, load_sem.at[3]) for src, dst in ((q_hbm, q), (g_hbm, g))]
    load_k.start()
    load_v.start()
    barrier = pltpu.get_barrier_semaphore()
    for o in (1, 2):
        pl.semaphore_signal(
            barrier, inc=1, device_id={"ctx": partner(me, o, n)}, device_id_type=MESH)
    load_span.start()
    for load in load_qg:
        load.start()
    rank[...] = lax.broadcasted_iota(jnp.int32, rank.shape, 0) - (
        lax.broadcasted_iota(jnp.int32, rank.shape, 1) // cluster)

    def remote(src, dst, sem, to):
        return pltpu.make_async_remote_copy(
            src_ref=src, dst_ref=dst, send_sem=sent.at[0], recv_sem=sem,
            device_id={"ctx": partner(me, to, n)}, device_id_type=MESH)

    def landed(ref, sem):
        pltpu.make_async_copy(ref, ref, sem).wait()

    def cut(h, c=0, pieces=1):
        size = half_rows // pieces
        return pl.ds(h * half_rows + c * size, size)

    def direct_first(o, which, c):
        at = cut(o - 1, c, pieces_of[which])
        return remote(kv.at[0, which, at], kv.at[o, which, at], first.at[which, o - 1, c], o)

    def direct_second(o, which):
        at = cut(2 - o)
        return remote(kv.at[0, which, at], kv.at[o, which, at], second.at[which], o)

    def relay(o, which, c):
        at = cut(2 - o, c, pieces_of[which])
        return remote(kv.at[3 - o, which, at], kv.at[3, which, at], third.at[which], o)

    def pass_gathered(which):
        for c in range(pieces_of[which]):
            for o in (1, 2):
                direct_first(3 - o, which, c).wait_recv()
                relay(o, which, c).start()

    def place(j):
        return pl.ds(j * slot_rows, slot_rows)

    def line(o, j):
        return pl.ds(o * slots_here + j, 1)

    def raw_scores(c, o, j):
        return dot(kv[o, 0, place(j)], q[pl.ds(c * chunk, chunk), :], ((1,), (1,)))

    def soften(c, o, j, piece):
        span = pl.ds(c * chunk, chunk)
        i = (c * chunk) // slot_cols
        shift = ((c * chunk) % slot_cols) // cluster
        diagonal = o == 0 and j == i
        if diagonal:
            piece = jnp.where(rank[...] <= shift, piece, NEGATIVE)
        peak = jnp.max(piece, axis=0, keepdims=True)
        e = jnp.exp2((piece - peak) * scale2)
        total[line(o, j), span] = jnp.sum(e, axis=0, keepdims=True)
        p[o, place(j), span] = e.astype(p.dtype)
        peak = peak * scale2
        if not diagonal:
            visible = span_ref[partner(me, o, n) * slots_here + j] < span_ref[me * slots_here + i]
            peak = jnp.where(visible, peak, NEGATIVE)
        top[line(o, j), span] = peak

    def scores(*blocks):
        for c in range(chunks):
            for o in blocks:
                for j in range(slots_here):
                    soften(c, o, j, raw_scores(c, o, j))

    def weigh(c, o):
        span = pl.ds(c * chunk, chunk)
        t = top[:, span]
        factor = jnp.exp2(t - jnp.max(t, axis=0, keepdims=True))
        weight = factor / jnp.sum(factor * total[:, span], axis=0, keepdims=True)
        top[:, span] = weight
        shares = []
        for j in range(slots_here):
            at = o * slots_here + j
            w = (p[o, place(j), span].astype(jnp.float32) * weight[at:at + 1]).astype(jnp.bfloat16)
            shares.append(dot(w, g[span, :], ((1,), (0,))))
        return shares

    def last_block(o):
        parts = None
        raw = [[raw_scores(c, o, j) for j in range(slots_here)] for c in range(chunks)]
        for c in range(chunks):
            for j in range(slots_here):
                soften(c, o, j, raw[c][j])
        for c in range(chunks):
            shares = weigh(c, o)
            parts = shares if parts is None else [a + b for a, b in zip(parts, shares)]
        return parts

    def products(*blocks):
        for c in range(chunks):
            span = pl.ds(c * chunk, chunk)
            for o in blocks:
                for j in range(slots_here):
                    d = dot(kv[o, 1, place(j)], g[span, :], ((1,), (1,)))
                    dsum[line(o, j), span] = jnp.sum(p[o, place(j), span].astype(jnp.float32) * d, axis=0, keepdims=True)
                    dp[o, place(j), span] = d

    def value_parts(*blocks):
        for c in range(chunks):
            span = pl.ds(c * chunk, chunk)
            for i, o in enumerate(blocks):
                for j in range(slots_here):
                    w = p[o, place(j), span].astype(jnp.float32) * top[line(o, j), span]
                    pb[i, place(j), span] = w.astype(jnp.bfloat16)
        return [[dot(pb[i, place(j)], g[...], ((1,), (0,))) for j in range(slots_here)]
                for i in range(len(blocks))]

    def key_parts(*blocks):
        for c in range(chunks):
            span = pl.ds(c * chunk, chunk)
            for o in blocks:
                for j in range(slots_here):
                    w = p[o, place(j), span].astype(jnp.float32) * top[line(o, j), span]
                    ds[o, place(j), span] = (
                        w * (dp[o, place(j), span] - delta[:, span])).astype(jnp.bfloat16)
        return [[dot(ds[o, place(j)], q[...], ((1,), (0,))) * scale for j in range(slots_here)]
                for o in blocks]

    def back_whole(o, which):
        return remote(part.at[o, which], recv.at[o, which], home.at[which], o)

    def back_piece(o, which, h, c=0, pieces=1):
        at = cut(h, c, pieces)
        return remote(part.at[o, which, at], recv.at[o, which, at], home.at[which], o)

    def back_diagonal(which, h, c):
        size = half_rows // BACK_PIECES
        return remote(part.at[3, which, cut(h, c, BACK_PIECES)],
                      passing.at[which, c, pl.ds(h * size, size)], pass_sem.at[which, c], 1 + h)

    def leave(which, direct, blocks, parts):
        sends = []
        for o, block in zip(blocks, parts):
            if direct or o == 3:
                for j in range(slots_here):
                    part[o, which, place(j)] = block[j].astype(part.dtype)
                sends += [back_whole(o, which)] if direct else [
                    back_diagonal(which, h, c) for c in range(BACK_PIECES) for h in (0, 1)]
            else:
                block = jnp.concatenate(block, axis=0)
                now, later = o - 1, 2 - o
                part[o, which, cut(now)] = block[now * half_rows:(now + 1) * half_rows].astype(part.dtype)
                held[o - 1, which] = block[later * half_rows:(later + 1) * half_rows]
                sends.append(back_piece(o, which, now))
        for send in sends:
            send.start()

    def pass_on(which):
        size = half_rows // BACK_PIECES
        for c in range(BACK_PIECES):
            landed(passing.at[which, c], pass_sem.at[which, c])
            for o in (1, 2):
                h = 2 - o
                part[o, which, cut(h, c, BACK_PIECES)] = (
                    held[o - 1, which, pl.ds(c * size, size)]
                    + passing[which, c, pl.ds(h * size, size)].astype(jnp.float32)).astype(part.dtype)
            for o in (1, 2):
                back_piece(o, which, 2 - o, c, BACK_PIECES).start()

    def store_own(which, block):
        for j in range(slots_here):
            acc[which, place(j)] = block[j]

    def plan(direct):
        pl.semaphore_wait(barrier, 2)
        for which, load in ((0, load_k), (1, load_v)):
            load.wait()
            for c in range(pieces_of[which]):
                for o in (1, 2):
                    direct_first(o, which, c).start()
        for which in range(2):
            for o in (1, 2):
                direct_second(o, which).start()
        load_span.wait()
        landed(qg, load_sem.at[3])
        scores(0)
        products(0)
        pass_gathered(0)
        pass_gathered(1)
        landed(kv.at[0, 0], second.at[0])
        scores(1, 2)
        landed(kv.at[0, 1], second.at[1])
        products(1, 2)
        landed(kv.at[3, 0], third.at[0])
        leave(1, direct[1], (3,), [last_block(3)])
        leave(1, direct[1], (1, 2), value_parts(1, 2))
        landed(kv.at[3, 1], third.at[1])
        products(3)
        delta[...] = jnp.sum(top[...] * dsum[...], axis=0, keepdims=True)
        leave(0, direct[0], (3,), key_parts(3))
        leave(0, direct[0], (1, 2), key_parts(1, 2))
        store_own(1, value_parts(0)[0])
        if not direct[1]:
            pass_on(1)
        store_own(0, key_parts(0)[0])
        if not direct[0]:
            pass_on(0)
        for c in range(chunks):
            span = pl.ds(c * chunk, chunk)
            sofar = jnp.zeros((head_dim, chunk), jnp.float32)
            for o in range(n):
                sofar = sofar + dot(kv[o, 0], ds[o, :, span], ((0,), (0,)))
            dq_ref[span, :] = (sofar.T * scale).astype(dq_ref.dtype)

        for which, out in ((1, dv_ref), (0, dk_ref)):
            count = 3 if direct[which] else 2
            landed(recv.at[pl.ds(1, count), which], home.at[which])
            whole = acc[which]
            for o in range(1, count + 1):
                whole = whole + recv[o, which].astype(jnp.float32)
            out[...] = whole.astype(out.dtype)
        landed(dp.at[0, pl.ds(0, 12 * rows * head_dim * 2 // (4 * cols))], sent.at[0])

    lower = lax.axis_index("seq") % 2 == 0
    pl.when(lower)(lambda: plan((True, False)))
    pl.when(jnp.logical_not(lower))(lambda: plan((False, False)))


def kernel(n, cluster, slots_here, chunk, keep, span_hbm, q_hbm, g_hbm, k_hbm, v_hbm,
           dq_ref, dk_ref, dv_ref,
           q, g, kv, p, dp, ds, pb, part, recv, top, total, dsum, delta, rank, acc, span_ref,
           load_sem, send_sem, recv_sem, back_send, back_recv):
    me = lax.axis_index("ctx")
    rows = kv.shape[2]
    slot_rows = rows // slots_here
    cols = q.shape[0]
    slot_cols = slot_rows * cluster
    chunks = cols // chunk
    scale = 1.0 / math.sqrt(q.shape[1])
    scale2 = scale * math.log2(math.e)

    loads = [
        pltpu.make_async_copy(src, dst, load_sem.at[i])
        for i, (src, dst) in enumerate(
            [(k_hbm, kv.at[0, 0]), (v_hbm, kv.at[0, 1]), (q_hbm, q), (g_hbm, g),
             (span_hbm, span_ref)]
        )
    ]
    for load in loads:
        load.start()
    barrier = pltpu.get_barrier_semaphore()
    each(1, n, lambda o: pl.semaphore_signal(
        barrier, inc=1, device_id={"ctx": partner(me, o, n)}, device_id_type=MESH))
    rank[...] = lax.broadcasted_iota(jnp.int32, rank.shape, 0) - (
        lax.broadcasted_iota(jnp.int32, rank.shape, 1) // cluster)

    def remote(src, dst, sems, o, which):
        return pltpu.make_async_remote_copy(
            src_ref=src, dst_ref=dst,
            send_sem=sems[0].at[o, which], recv_sem=sems[1].at[o, which],
            device_id={"ctx": partner(me, o, n)}, device_id_type=MESH)

    there, home = (send_sem, recv_sem), (back_send, back_recv)

    def gather(o, which):
        return remote(kv.at[0, which], kv.at[o, which], there, o, which)

    def back(o, which):
        return remote(part.at[o, which], recv.at[o, which], home, o, which)

    def scores(o):
        source = partner(me, o, n)
        for c in range(chunks):
            span = pl.ds(c * chunk, chunk)
            s = dot(kv[o, 0], q[span, :], ((1,), (1,))) * scale2
            own = span_ref[me * slots_here + (c * chunk) // slot_cols]
            shift = ((c * chunk) % slot_cols) // cluster
            pieces = []
            for j in range(slots_here):
                limit = (own - span_ref[source * slots_here + j]) * slot_rows + shift
                pieces.append(jnp.where(
                    rank[...] <= limit, s[j * slot_rows:(j + 1) * slot_rows], NEGATIVE))
            s = jnp.concatenate(pieces, axis=0)
            m = jnp.max(s, axis=0, keepdims=True)
            e = jnp.exp2(s - m)
            top[o, :, span] = m
            total[o, :, span] = jnp.sum(e, axis=0, keepdims=True)
            p[o, :, span] = e.astype(p.dtype)

    def products(o):
        for c in range(chunks):
            span = pl.ds(c * chunk, chunk)
            d = dot(kv[o, 1], g[span, :], ((1,), (1,)))
            dsum[o, :, span] = jnp.sum(p[o, :, span].astype(jnp.float32) * d, axis=0, keepdims=True)
            if keep:
                dp[o, :, span] = d

    def normalize():
        factor = jnp.exp2(top[...] - jnp.max(top[...], axis=0)[None])
        whole = jnp.sum(factor * total[...], axis=0)
        top[...] = factor / whole[None]

    def value_part(o):
        for c in range(chunks):
            span = pl.ds(c * chunk, chunk)
            w = p[o, :, span].astype(jnp.float32) * top[o, :, span]
            pb[:, span] = w.astype(jnp.bfloat16)
        return dot(pb[...], g[...], ((1,), (0,)))

    def key_part(o):
        for c in range(chunks):
            span = pl.ds(c * chunk, chunk)
            w = p[o, :, span].astype(jnp.float32) * top[o, :, span]
            d = dp[o, :, span] if keep else dot(kv[o, 1], g[span, :], ((1,), (1,)))
            ds[o, :, span] = (w * (d - delta[:, span])).astype(jnp.bfloat16)
        return dot(ds[o], q[...], ((1,), (0,))) * scale

    def leave(o, which):
        part[o, which] = (key_part, value_part)[which](o).astype(part.dtype)
        back(o, which).start()

    pl.semaphore_wait(barrier, n - 1)
    for which in range(2):
        loads[which].wait()
        each(1, n, lambda o: gather(o, which).start())
    loads[4].wait()
    loads[2].wait()
    loads[3].wait()
    scores(0)
    products(0)

    def arrive(o):
        gather(o, 0).wait_recv()
        scores(o)
        gather(o, 1).wait_recv()
        products(o)

    each(1, n, arrive)
    normalize()
    each(1, n, lambda i: leave(n - i, 1))
    delta[...] = jnp.sum(top[...] * dsum[...], axis=0)
    each(1, n, lambda i: leave(n - i, 0))
    acc[1] = value_part(0)
    acc[0] = key_part(0)

    for c in range(chunks):
        span = pl.ds(c * chunk, chunk)

        def add(o, sofar):
            return sofar + dot(kv[o, 0], ds[o, :, span], ((0,), (0,)))

        sofar = jnp.zeros((q.shape[1], chunk), jnp.float32)
        if n <= 4:
            for o in range(n):
                sofar = add(o, sofar)
        else:
            sofar = lax.fori_loop(0, n, add, sofar)
        dq_ref[span, :] = (sofar.T * scale).astype(dq_ref.dtype)

    def collect(which):
        def one(o):
            back(o, which).wait_recv()
            acc[which] += recv[o, which].astype(jnp.float32)

        each(1, n, one)

    collect(1)
    dv_ref[...] = acc[1].astype(dv_ref.dtype)
    collect(0)
    dk_ref[...] = acc[0].astype(dk_ref.dtype)

    def finish(o):
        for which in range(2):
            gather(o, which).wait_send()
            back(o, which).wait_send()

    each(1, n, finish)


def store(dq, dk, dv, dq_out, dk_out, dv_out, sem):
    copies = [
        pltpu.make_async_copy(src, dst, sem.at[i])
        for i, (src, dst) in enumerate([(dq, dq_out), (dk, dk_out), (dv, dv_out)])
    ]
    for copy in copies:
        copy.start()
    for copy in copies:
        copy.wait()


def local(queries, key_rows, value_slot_rows, out_grad, span_order):
    rows, query_local, head_dim = queries.shape
    kv_local = key_rows.shape[1]
    assert kv_local == 1
    n = lax.axis_size("ctx")
    slots_here = span_order.shape[0] // n
    cluster = query_local // kv_local
    cols = rows * cluster
    chunk = math.gcd(256, cols // slots_here)
    keep = n <= 8
    slot_rows = rows // slots_here
    any_spec = pl.BlockSpec(memory_space=pl.ANY)
    vmem_spec = pl.BlockSpec(memory_space=pltpu.VMEM)
    bf16, f32 = jnp.bfloat16, jnp.float32
    pair = (n, 2, rows, head_dim)
    stat = (n * slots_here, cols) if n == 4 else (n, 1, cols)
    both = [pltpu.VMEM((2, cols, head_dim), bf16)] if n == 4 else [pltpu.VMEM((cols, head_dim), bf16)] * 2
    buffers = both + [
        pltpu.VMEM(pair, bf16),
        pltpu.VMEM((n, rows, cols), f32 if keep and n != 4 else bf16),
        pltpu.VMEM((n, rows, cols) if keep else (1, 8, 128), f32),
        pltpu.VMEM((n, rows, cols), bf16),
        pltpu.VMEM((2, rows, cols) if n == 4 else (rows, cols), bf16),
        pltpu.VMEM(pair, bf16),
        pltpu.VMEM(pair, bf16),
    ]
    sums = [
        pltpu.VMEM(stat, f32),
        pltpu.VMEM(stat, f32),
        pltpu.VMEM(stat, f32),
        pltpu.VMEM((1, cols), f32),
        pltpu.VMEM((slot_rows, chunk), jnp.int32),
        pltpu.VMEM((2, rows, head_dim), f32),
        pltpu.SMEM(span_order.shape, jnp.int32),
    ]
    dma = pltpu.SemaphoreType.DMA
    if n == 4:
        body = functools.partial(square, cluster, slots_here, chunk)
        scratch = buffers + [
            pltpu.VMEM((2, BACK_PIECES, rows // BACK_PIECES, head_dim), bf16),
            pltpu.VMEM((2, 2, rows // 2, head_dim), f32),
        ] + sums + [
            dma((4,)), dma((1,)), dma((2, 2, max(KEY_PIECES, VALUE_PIECES))), dma((2,)), dma((2,)),
            dma((2, BACK_PIECES)), dma((2,)),
        ]
    else:
        body = functools.partial(kernel, n, cluster, slots_here, chunk, keep)
        scratch = buffers + sums + [dma((5,))] + [dma((n, 2))] * 4
    dq, dk, dv = pl.pallas_call(
        body,
        out_shape=(
            pltpu.VMEM((cols, head_dim), bf16),
            pltpu.VMEM((rows, head_dim), bf16),
            pltpu.VMEM((rows, head_dim), bf16),
        ),
        in_specs=[any_spec] * 5,
        out_specs=(vmem_spec,) * 3,
        scratch_shapes=scratch,
        compiler_params=pltpu.CompilerParams(
            collective_id=0, has_side_effects=True, vmem_limit_bytes=60 * 1024 * 1024
        ),
    )(
        span_order,
        queries.reshape(cols, head_dim),
        out_grad.reshape(cols, head_dim),
        key_rows.reshape(rows, head_dim),
        value_slot_rows.reshape(rows, head_dim),
    )
    dq, dk, dv = pl.pallas_call(
        store,
        out_shape=tuple(jax.ShapeDtypeStruct(a.shape, bf16) for a in (dq, dk, dv)),
        in_specs=[vmem_spec] * 3,
        out_specs=(any_spec,) * 3,
        scratch_shapes=[pltpu.SemaphoreType.DMA((3,))],
    )(*(pltpu.with_memory_space_constraint(a, pltpu.VMEM) for a in (dq, dk, dv)))
    return dq.reshape(queries.shape), dk.reshape(key_rows.shape), dv.reshape(key_rows.shape)


def solution(mesh):
    rows = P(("seq", "ctx"), "tp", None)
    return jax.shard_map(
        local,
        mesh=mesh,
        in_specs=(rows, rows, rows, rows, P("seq")),
        out_specs=(rows, rows, rows),
        check_vma=False,
    )
```
